256 devices in a mesh: feat: 8 (over x, core), rows: 32 (over z, y).
Axes of the slice: x: 4, y: 4, z: 8, core: 2. Of those that a mesh axis runs over, the one named last changes fastest.
Arguments:
- acts: bfloat16 [32768, 16384], P('rows', 'feat'), may hold values from -6 to 6
- grads_out: bfloat16 [32768, 16384], P('rows', 'feat'), may hold values from -0.59765625 to 0.59765625
- proj_in: bfloat16 [16384, 128], P('feat'), may hold values from -0.046875 to 0.046875
- proj_out: bfloat16 [16384, 128], P('feat'), may hold values from -0.046875 to 0.046875
- doc_ids: int32 [32768], P('rows'), may hold values from -1 to 127, as said below
- block_counts: int32 [128], replicated, may hold values from 1 to 65, as said below
- inverse_dense: bfloat16 [16384, 16384], P('rows', 'feat'), may hold values from -0.046875 to 0.046875
- inverse_diag: float32 [16384], P('rows'), may hold values from 0.5 to 2
- train_grads: bfloat16 [16384, 16384], P('rows', 'feat'), may hold values from -0.046875 to 0.046875
Outputs:
- scores: float32 [128, 16384], P('feat', 'rows')
The draws below stay inside these ranges and needn't reach their ends.
Inputs may be any that keep to these rules, and one draw needn't show every extreme that they name: `doc_ids`: documents are laid end to end in order, document d over block_counts_d whole blocks of 128 tokens; its tokens come first and the rest of its last block is padding with id -1; every block holds real tokens of its document. `block_counts`: the counts sum to 256; one document has exactly the most.
All inputs are finite; a program needn't handle non-finite values.
Results may differ from the reference program's by a relative error of at most 0.0057.
Values may be sent and summed in bfloat16 or wider, within the bound.
A program may use at most 64 MiB of HBM per device.

```python
import math
import jax
import jax.numpy as jnp
from jax import lax

D = 16384
K = 128
BLOCK = 128
TOKENS = 32768
NBLK = 256
DOCS = 128
NTRAIN = 16384
F = 16384


def layout(key):
    base = jax.random.fold_in(key, 7)
    first, second, third = jax.random.split(base, 3)
    spare = NBLK - DOCS
    heavy = (spare + 1) // 2
    rest = spare - heavy
    chosen = jax.random.randint(third, (), 0, DOCS)
    picks = jax.random.randint(first, (max(rest, 1),), 0, DOCS - 1)
    picks = jnp.where(picks >= chosen, picks + 1, picks)
    valid = (jnp.arange(max(rest, 1), dtype=jnp.int32) < rest).astype(jnp.int32)
    docs_all = jnp.arange(DOCS, dtype=jnp.int32)
    spread = jnp.sum((picks[:, None] == docs_all[None, :]).astype(jnp.int32) * valid[:, None], axis=0)
    counts = 1 + spread + jnp.where(docs_all == chosen, heavy, 0)
    pads = jax.random.randint(second, (DOCS,), 0, BLOCK)
    return (counts.astype(jnp.int32), pads.astype(jnp.int32))


def draw_block_counts(key, part):
    counts, pads = layout(key)
    return counts


def draw_doc_ids(key, part):
    counts, pads = layout(key)
    starts = jnp.cumsum(counts) - counts
    places = jnp.arange(NBLK, dtype=jnp.int32)
    owner = jnp.sum((starts[None, :] <= places[:, None]).astype(jnp.int32), axis=1) - 1
    position = jnp.arange(TOKENS, dtype=jnp.int32)
    docs_here = owner[position // BLOCK]
    offset = position - starts[docs_here] * BLOCK
    length = counts[docs_here] * BLOCK - pads[docs_here]
    return jnp.where(offset < length, docs_here, -1).astype(jnp.int32)


def steps_of(key, dims, pieces, smallest, high):
    def one(axis_at, parts):
        draws = jax.random.uniform(jax.random.fold_in(jax.random.fold_in(key, 6), axis_at), (parts,), jnp.float32, smallest / len(pieces), high / len(pieces))
        return jnp.repeat(jnp.exp(draws), dims[axis_at] // parts).reshape((-1,) + (1,) * (len(dims) - axis_at - 1))

    factor_of = one(*pieces[0])
    for cut in pieces[1:]:
        factor_of = factor_of * one(*cut)
    return factor_of


def normal_values(stream_key, dims, scale, bound, pieces=(), held_as=jnp.bfloat16):
    result = scale * jax.random.normal(stream_key, dims, jnp.float32)
    if pieces:
        result = result * steps_of(stream_key, dims, pieces, -0.22, 0.18)
    return jnp.clip(result, -bound, bound).astype(held_as)


def setup_inputs(seed: int = 0) -> dict:
    key_list = jax.random.split(jax.random.key(seed), 10)
    return {
        "acts": normal_values(key_list[0], (TOKENS, D), 1.0, 6.0, ((0, 32), (1, 8))),
        "grads_out": normal_values(key_list[1], (TOKENS, D), 0.1, 0.59765625, ((0, 32), (1, 8))),
        "proj_in": normal_values(key_list[2], (D, K), D ** -0.5, 0.046875, ((0, 8),)),
        "proj_out": normal_values(key_list[3], (D, K), D ** -0.5, 0.046875, ((0, 8),)),
        "doc_ids": draw_doc_ids(jax.random.fold_in(key_list[9], 71), 0),
        "block_counts": draw_block_counts(jax.random.fold_in(key_list[9], 71), 0),
        "inverse_dense": normal_values(key_list[6], (F, F), F ** -0.5, 0.046875, ((0, 32), (1, 8))),
        "inverse_diag": jnp.clip(jnp.exp(math.log(2.0) - 1.3862944 * jax.random.uniform(key_list[7], (F,), jnp.float32) ** steps_of(key_list[7], (F,), ((0, 32),), -0.2, 0.2)), 0.5, 2.0),
        "train_grads": normal_values(key_list[8], (NTRAIN, F), F ** -0.5, 0.046875, ((0, 32), (1, 8))),
    }


def owners(block_counts):
    starts = jnp.cumsum(block_counts) - block_counts
    places = jnp.arange(NBLK, dtype=jnp.int32)
    return jnp.sum((starts[None, :] <= places[:, None]).astype(jnp.int32), axis=1) - 1


def reference(acts, grads_out, proj_in, proj_out, doc_ids, block_counts, inverse_dense, inverse_diag, train_grads):
    xin = jnp.dot(acts, proj_in, preferred_element_type=jnp.float32).astype(jnp.bfloat16)
    gout = jnp.dot(grads_out, proj_out, preferred_element_type=jnp.float32).astype(jnp.bfloat16)
    owner = owners(block_counts)
    tok_owner = jnp.repeat(owner, BLOCK)
    gmask = jnp.where((doc_ids == tok_owner)[:, None], gout, jnp.zeros_like(gout))
    left = gmask.astype(jnp.float32).reshape(NBLK, BLOCK, K)
    right = xin.astype(jnp.float32).reshape(NBLK, BLOCK, K)
    blocksum = jnp.einsum("kta,ktc->kac", left, right).reshape(NBLK, K * K)
    member = (owner[None, :] == jnp.arange(DOCS, dtype=jnp.int32)[:, None]).astype(jnp.float32)
    summed = jnp.dot(member, blocksum, precision=lax.Precision.HIGHEST)
    docgrad = (summed / block_counts.astype(jnp.float32)[:, None]).astype(jnp.bfloat16)
    dense = jnp.dot(docgrad, inverse_dense, preferred_element_type=jnp.float32)
    precond = (dense + docgrad.astype(jnp.float32) * inverse_diag[None, :]).astype(jnp.bfloat16)
    return jnp.dot(precond, train_grads.T, preferred_element_type=jnp.float32)
```

```python
import jax
import jax.numpy as jnp
from jax import lax
from jax.experimental import pallas as pl
from jax.experimental.pallas import tpu as pltpu
from jax.sharding import PartitionSpec as P

BF = jnp.bfloat16
F32 = jnp.float32
I32 = jnp.int32

NX, NC, NY, NZ = 4, 2, 4, 8
NF = NX * NC
NR = NZ * NY
BLOCK = 128
K = 128
DOCS = 128
X_ORDER = (2, 1, 3, 0)
Y_FAR = (2, 1, 3)
Y_NEAR = (1, 3, 2)
Z_FAR = (4, 3, 5, 2, 6, 1, 7)
Z_NEAR = (1, 7, 2, 6, 3, 5, 4)
F_FAR = (4, 5, 3, 2, 6, 7, 1)
X_DT = BF
D_DT = F32


def iota(shape, dim):
    return lax.broadcasted_iota(I32, shape, dim)


def one_hot_rows(source_of):
    q = iota((K, K), 0)
    return (iota((K, K), 1) == source_of(q)).astype(F32).astype(BF)


def dot(a, b):
    return jnp.dot(a, b, preferred_element_type=F32)


def dot_nt(a, b):
    return lax.dot_general(a, b, (((1,), (1,)), ((), ())), preferred_element_type=F32)


def kernel(
    acts, grads, pin, pout, ids, counts, inv, diag, train,
    out,
    acts_v, grads_v, pin_v, pout_v, ids_v, counts_v, inv_v, diag_v, train_v,
    member, perms, columns,
    pa, sib, xs, xr, s1, r1, s2, r2, ags, ag, dg, s3, r3, own, s4, r4, pc, acc, s5, r5,
    in_sem, chunk_sem,
    sib_send, sib_recv, x_send, x_recv, b1_send, b1_recv, b2_send, b2_recv,
    ag_send, ag_recv, c1_send, c1_recv, c2_send, c2_recv, p1_send, p1_recv,
    p2_send, p2_recv, d_send, d_recv,
):
    f = lax.axis_index("feat")
    r = lax.axis_index("rows")
    x, c = f // NC, f % NC
    z, y = r // NY, r % NY

    def feat_at(k):
        return {"feat": lax.rem(f + k, NF)}

    def y_at(k):
        return lax.rem(y + k, NY)

    def z_at(k):
        return lax.rem(z + k, NZ)

    def rows_peer(zp, yp):
        return {"rows": zp * NY + yp}

    sibling = {"feat": x * NC + (1 - c)}

    loads = [
        pltpu.make_async_copy(counts, counts_v, in_sem.at[0]),
        pltpu.make_async_copy(ids, ids_v, in_sem.at[1]),
        pltpu.make_async_copy(pin, pin_v, in_sem.at[2]),
        pltpu.make_async_copy(pout, pout_v, in_sem.at[3]),
    ]
    for copy in loads:
        copy.start()
    chunk = {}
    for k in X_ORDER:
        at = pl.ds(pl.multiple_of(lax.rem(x + k, NX) * 256, 256), 256)
        chunk[k] = (
            pltpu.make_async_copy(acts.at[at, :], acts_v.at[k], chunk_sem.at[0, k]),
            pltpu.make_async_copy(grads.at[at, :], grads_v.at[k], chunk_sem.at[1, k]),
        )
        for copy in chunk[k]:
            copy.start()
    late = [pltpu.make_async_copy(diag, diag_v, in_sem.at[4])]
    for k in range(NY):
        at = pl.ds(pl.multiple_of(y_at(k) * 512, 512), 512)
        late.append(pltpu.make_async_copy(inv.at[:, at], inv_v.at[k], in_sem.at[5 + k]))
    for k in range(NY):
        at = pl.ds(pl.multiple_of(y_at(NY - k) * 512, 512), 512)
        late.append(pltpu.make_async_copy(train.at[:, at], train_v.at[k], in_sem.at[9 + k]))
    for copy in late:
        copy.start()

    barrier = pltpu.get_barrier_semaphore()
    for k in range(1, NF):
        pl.semaphore_signal(barrier, inc=1, device_id=feat_at(k))
    for k in Y_FAR:
        pl.semaphore_signal(barrier, inc=1, device_id=rows_peer(z, y_at(k)))
    for k in Z_FAR:
        pl.semaphore_signal(barrier, inc=1, device_id=rows_peer(z_at(k), y))

    loads[0].wait()
    loads[1].wait()
    doc, lane = iota((K, K), 0), iota((K, K), 1)
    count_row = jnp.broadcast_to(counts_v[...].astype(F32), (K, K))
    start = jnp.sum(jnp.where(lane < doc, count_row, 0.0), axis=1, keepdims=True)
    count = jnp.sum(jnp.where(lane == doc, count_row, 0.0), axis=1, keepdims=True)
    q = iota((DOCS, NF * NR), 1)
    block = (((q & 31) << 3) | (q >> 5)).astype(F32)
    member[...] = jnp.where((start <= block) & (block < start + count), 1.0, 0.0).astype(BF)
    mine = (r * NF + f).astype(F32)
    owner = jnp.sum(jnp.where(start <= mine, 1.0, 0.0), axis=0, keepdims=True) - 1.0
    same = jnp.where(ids_v[pl.ds(f, 1), :].astype(F32) == owner, 1.0, 0.0)
    keep = jnp.sum(jnp.where(lane == doc, jnp.broadcast_to(same, (K, K)), 0.0), axis=1, keepdims=True)
    columns[0] = jnp.broadcast_to(keep, (K, K))
    columns[1] = jnp.broadcast_to(count, (K, K))
    perms[0] = one_hot_rows(lambda q: ((q >> 2) & 7) * 16 + (q >> 5) * 4 + (q & 3))
    perms[1] = one_hot_rows(lambda q: ((q >> 2) & 3) * 32 + (q >> 4) * 4 + (q & 3))
    perms[2] = one_hot_rows(lambda q: ((q >> 2) & 7) * 16 + (q & 3) * 4 + (q >> 5))

    sends = []

    def send(src, dst, ssem, rsem, device):
        copy = pltpu.make_async_remote_copy(
            src_ref=src, dst_ref=dst, send_sem=ssem, recv_sem=rsem,
            device_id=device, device_id_type=pl.DeviceIdType.MESH,
        )
        copy.start()
        sends.append(copy)
        return copy

    mine_at = pl.ds(pl.multiple_of(c * BLOCK, BLOCK), BLOCK)
    theirs_at = pl.ds(pl.multiple_of((1 - c) * BLOCK, BLOCK), BLOCK)
    from_sib, from_x = {}, {}

    def project(k):
        chunk[k][0].wait()
        pa[k, :, 0:K] = dot(acts_v[k], pin_v[...])
        chunk[k][1].wait()
        pa[k, :, K:2 * K] = dot(grads_v[k], pout_v[...])

    def to_sibling(k):
        from_sib[k] = send(pa.at[k, theirs_at, :], sib.at[k], sib_send.at[k], sib_recv.at[k], sibling)

    def to_owner(k):
        from_sib[k].wait_recv()
        xs[k] = (pa[k, mine_at, :] + sib[k]).astype(X_DT)
        device = {"feat": lax.rem(x + k, NX) * NC + c}
        from_x[k] = send(xs.at[k], xr.at[k], x_send.at[k], x_recv.at[k], device)

    loads[2].wait()
    loads[3].wait()
    project(2)
    pl.semaphore_wait(barrier, NF - 1 + len(Y_FAR) + len(Z_FAR))
    to_sibling(2)
    project(1)
    to_sibling(1)
    to_owner(2)
    project(3)
    to_sibling(3)
    to_owner(1)
    project(0)
    to_sibling(0)
    to_owner(3)
    from_sib[0].wait_recv()
    total = pa[0, mine_at, :] + sib[0]
    for k in (1, 3, 2):
        from_x[k].wait_recv()
        total = total + xr[k].astype(F32)

    xin = total[:, 0:K].astype(BF)
    gmask = jnp.where(columns[0] > 0.5, total[:, K:2 * K], 0.0).astype(BF)
    turned = dot_nt(perms[0], gmask).astype(BF)
    blocksum = dot(turned, xin).astype(BF)
    for k in range(NY):
        s1[k] = blocksum[32 * k:32 * k + 32]
    got = {}
    for k in Y_FAR:
        got[k] = send(s1.at[y_at(k)], r1.at[y], b1_send.at[k], b1_recv.at[k], rows_peer(z, y_at(k)))
    r1[y] = s1[y]
    for k in Y_NEAR:
        got[k].wait_recv()
    second = dot(perms[1], r1[...].reshape(K, K)).astype(BF)
    for k in range(NZ):
        s2[k] = second[16 * k:16 * k + 16]
    for k in Z_FAR:
        got[k] = send(s2.at[z_at(k)], r2.at[z], b2_send.at[k], b2_recv.at[k], rows_peer(z_at(k), y))
    r2[z] = s2[z]
    for k in Z_NEAR:
        got[k].wait_recv()
    third = dot(perms[2], r2[...].reshape(K, K)).astype(BF)
    ag_at = pl.ds(pl.multiple_of(f * NR, NR), NR)
    for k in range(4):
        ags[k] = third[NR * k:NR * k + NR]
    for k in F_FAR:
        got[k] = send(ags, ag.at[:, ag_at, :], ag_send.at[k], ag_recv.at[k], feat_at(k))
    for k in range(4):
        ag[k, ag_at, :] = third[NR * k:NR * k + NR]
    for copy in late:
        copy.wait()
    for k in F_FAR[::-1]:
        got[k].wait_recv()

    for k in range(4):
        dg[:, K * k:K * k + K] = (dot(member[...], ag[k]) / columns[1]).astype(BF)

    for k in Y_FAR:
        s3[k] = dot(dg[...], inv_v[k]).astype(BF)
        got[k] = send(s3.at[k], r3.at[k], c1_send.at[k], c1_recv.at[k], rows_peer(z, y_at(k)))
    own[...] = dot(dg[...], inv_v[0])
    for k in range(4):
        at = slice(K * k, K * k + K)
        own[:, at] += jnp.where(z == f, dg[:, at].astype(F32) * diag_v[k:k + 1, :], 0.0)
    for k in Y_NEAR:
        got[k].wait_recv()
    own[...] = own[...] + r3[1].astype(F32) + r3[3].astype(F32) + r3[2].astype(F32)
    s4[...] = own[...].astype(BF)
    for k in Z_FAR:
        at = pl.ds(pl.multiple_of(z_at(k) * 16, 16), 16)
        got[k] = send(s4.at[at, :], r4.at[k], c2_send.at[k], c2_recv.at[k], rows_peer(z_at(k), y))
    here = pl.ds(pl.multiple_of(z * 16, 16), 16)
    piece = own[here, :]
    for k in Z_NEAR:
        got[k].wait_recv()
        piece = piece + r4[k].astype(F32)
    pc[0, here, :] = piece.astype(BF)

    gather = {}

    def forward(at, j):
        for k in Y_FAR:
            copy = send(
                pc.at[0, at, :], pc.at[k, at, :], p2_send.at[j, k], p2_recv.at[k], rows_peer(z, y_at(k))
            )
        return copy

    for k in Z_FAR:
        gather[k] = send(
            pc.at[0, here, :], pc.at[0, here, :], p1_send.at[k], p1_recv.at[k], rows_peer(z_at(k), y)
        )
    forward(here, 0)
    for k in Z_NEAR:
        gather[k].wait_recv()
        forward(pl.ds(pl.multiple_of(z_at(NZ - k) * 16, 16), 16), k)
    acc[...] = dot_nt(pc[0], train_v[0])
    for k in Y_NEAR:
        pltpu.make_async_copy(pc.at[k], pc.at[k], p2_recv.at[k]).wait()
        acc[...] += dot_nt(pc[k], train_v[k])

    for k in range(NF):
        s5[k] = acc[16 * k:16 * k + 16, :].astype(D_DT)
    for k in F_FAR:
        got[k] = send(s5.at[lax.rem(f + k, NF)], r5.at[k], d_send.at[k], d_recv.at[k], feat_at(k))
    scores = acc[pl.ds(pl.multiple_of(f * 16, 16), 16), :]
    for k in F_FAR[::-1]:
        got[k].wait_recv()
        scores = scores + r5[k].astype(F32)
    out[...] = scores
    for copy in sends:
        copy.wait_send()


def per_device(acts, grads_out, proj_in, proj_out, doc_ids, block_counts, inverse_dense, inverse_diag, train_grads):
    def vmem(*shape, dtype=BF):
        return pltpu.VMEM(shape, dtype)

    dma = pltpu.SemaphoreType.DMA
    scratch = [
        vmem(4, 256, 2048), vmem(4, 256, 2048), vmem(2048, K), vmem(2048, K),
        vmem(8, 128, dtype=I32), vmem(1, 128, dtype=I32),
        vmem(4, 512, 512), vmem(4, 128, dtype=F32), vmem(4, 512, 512),
        vmem(DOCS, 256), vmem(3, K, K), vmem(2, K, K, dtype=F32),
        vmem(4, 256, 256, dtype=F32), vmem(4, 128, 256, dtype=F32),
        vmem(4, 128, 256, dtype=X_DT), vmem(4, 128, 256, dtype=X_DT),
        vmem(4, 32, K), vmem(4, 32, K), vmem(8, 16, K), vmem(8, 16, K),
        vmem(4, 32, K), vmem(4, 256, K), vmem(128, 512),
        vmem(4, 128, 512), vmem(4, 128, 512), vmem(128, 512, dtype=F32),
        vmem(128, 512), vmem(8, 16, 512), vmem(4, 128, 512), vmem(128, 512, dtype=F32),
        vmem(8, 16, 512, dtype=D_DT), vmem(8, 16, 512, dtype=D_DT),
        dma((13,)), dma((2, 4)),
        dma((4,)), dma((4,)), dma((4,)), dma((4,)), dma((4,)), dma((4,)), dma((8,)), dma((8,)),
        dma((8,)), dma((8,)), dma((4,)), dma((4,)), dma((8,)), dma((8,)), dma((8,)), dma((8,)),
        dma((8, 4)), dma((4,)), dma((8,)), dma((8,)),
    ]
    hbm = pl.BlockSpec(memory_space=pl.ANY)
    return pl.pallas_call(
        kernel,
        out_shape=jax.ShapeDtypeStruct((16, 512), F32),
        in_specs=[hbm] * 9,
        out_specs=pl.BlockSpec(memory_space=pltpu.VMEM),
        scratch_shapes=scratch,
        compiler_params=pltpu.CompilerParams(
            collective_id=0, has_side_effects=True, vmem_limit_bytes=60 * 1024 * 1024
        ),
        name="influence",
    )(
        acts, grads_out, proj_in, proj_out,
        doc_ids.reshape(8, 128), block_counts.reshape(1, 128),
        inverse_dense, inverse_diag.reshape(4, 128), train_grads,
    )


def solution(mesh):
    in_specs = (
        P("rows", "feat"),
        P("rows", "feat"),
        P("feat", None),
        P("feat", None),
        P("rows"),
        P(),
        P("rows", "feat"),
        P("rows"),
        P("rows", "feat"),
    )
    return jax.shard_map(
        per_device, mesh=mesh, in_specs=in_specs, out_specs=P("feat", "rows"), check_vma=False
    )
```

```python
import jax
import jax.numpy as jnp
from jax import lax
from jax.experimental import pallas as pl
from jax.experimental.pallas import tpu as pltpu
from jax.sharding import PartitionSpec as P

BF = jnp.bfloat16
F32 = jnp.float32
I32 = jnp.int32

NX, NC, NY, NZ = 4, 2, 4, 8
NF = NX * NC
NR = NZ * NY
BLOCK = 128
K = 128
DOCS = 128
Y_FAR = (2, 1, 3)
Y_NEAR = (1, 3, 2)
Z_FAR = (4, 3, 5, 2, 6, 1, 7)
Z_NEAR = (1, 7, 2, 6, 3, 5, 4)
F_FAR = (4, 5, 3, 2, 6, 7, 1)
X_FAR = (2, 1, 3)
R_FAR = sorted(
    ((dz, dy) for dz in range(NZ) for dy in range(NY) if dz or dy),
    key=lambda d: -min(d[0], NZ - d[0]) - min(d[1], NY - d[1]),
)
X_DT = BF
B_DT = BF
D_DT = BF


def iota(shape, dim):
    return lax.broadcasted_iota(I32, shape, dim)


def one_hot_rows(source_of):
    q = iota((K, K), 0)
    return (iota((K, K), 1) == source_of(q)).astype(F32).astype(BF)


def dot(a, b):
    return jnp.dot(a, b, preferred_element_type=F32)


def dot_nt(a, b):
    return lax.dot_general(a, b, (((1,), (1,)), ((), ())), preferred_element_type=F32)


def kernel(
    acts, grads, pin, pout, ids, counts, inv, diag, train,
    out,
    tokens_v, proj_v, ids_v, counts_v, inv_v, diag_v, train_v,
    member, perms, columns,
    pa, sib, xs, xr, s1, r1, ag, dg, s3, r3, own, s4, r4, pc, acc, s5, r5,
    in_sem, chunk_sem, plane,
    sib_send, sib_recv, x_send, x_recv, b1_send, b1_recv,
    ag_send, ag_recv, c1_send, c1_recv, c2_send, c2_recv, p1_send, p1_recv,
    p2_send, p2_recv, d_send, d_recv,
):
    f = lax.axis_index("feat")
    r = lax.axis_index("rows")
    x, c = f // NC, f % NC
    z, y = r // NY, r % NY

    def feat_at(k):
        return {"feat": lax.rem(f + k, NF)}

    def y_at(k):
        return lax.rem(y + k, NY)

    def z_at(k):
        return lax.rem(z + k, NZ)

    def rows_peer(zp, yp):
        return {"rows": zp * NY + yp}

    sibling = {"feat": x * NC + (1 - c)}

    projections = [
        pltpu.make_async_copy(pin, proj_v.at[0], in_sem.at[0]),
        pltpu.make_async_copy(pout, proj_v.at[1], in_sem.at[0]),
    ]
    for copy in projections:
        copy.start()

    def ahead(j):
        return jnp.where(j == 0, 2, jnp.where(j == 1, 1, jnp.where(j == 2, 3, 0)))

    def chunk(j):
        at = pl.ds(pl.multiple_of(lax.rem(x + ahead(j), NX) * 256, 256), 256)
        return (
            pltpu.make_async_copy(acts.at[at, :], tokens_v.at[j, 0], chunk_sem.at[j]),
            pltpu.make_async_copy(grads.at[at, :], tokens_v.at[j, 1], chunk_sem.at[j]),
        )

    for j in range(NX):
        for copy in chunk(j):
            copy.start()
    small = [
        pltpu.make_async_copy(counts, counts_v, in_sem.at[1]),
        pltpu.make_async_copy(ids, ids_v, in_sem.at[2]),
        pltpu.make_async_copy(diag, diag_v, in_sem.at[3]),
    ]
    late = []
    for k in range(NY):
        at = pl.ds(pl.multiple_of(y_at(k) * 512, 512), 512)
        late.append(pltpu.make_async_copy(inv.at[:, at], inv_v.at[k], in_sem.at[4]))
    for k in range(NY):
        at = pl.ds(pl.multiple_of(y_at(NY - k) * 512, 512), 512)
        late.append(pltpu.make_async_copy(train.at[:, at], train_v.at[k], in_sem.at[5]))

    barrier = pltpu.get_barrier_semaphore()
    for k in range(1, NF):
        pl.semaphore_signal(barrier, inc=1, device_id=feat_at(k))
    for k in Z_FAR:
        pl.semaphore_signal(barrier, inc=1, device_id=rows_peer(z_at(k), y))
    for k in Y_FAR:
        pl.semaphore_signal(barrier, inc=1, device_id=rows_peer(z, y_at(k)))

    sent = []

    def remote(src, dst, ssem, rsem, device):
        return pltpu.make_async_remote_copy(
            src_ref=src, dst_ref=dst, send_sem=ssem, recv_sem=rsem,
            device_id=device, device_id_type=pl.DeviceIdType.MESH,
        )

    def send(*args):
        copy = remote(*args)
        copy.start()
        return copy

    def wait_all(ref, sem):
        pltpu.make_async_copy(ref, ref, sem).wait()

    def finish():
        for ref, sem in sent:
            wait_all(ref, sem)

    mine_at = pl.ds(pl.multiple_of(c * BLOCK, BLOCK), BLOCK)
    theirs_at = pl.ds(pl.multiple_of((1 - c) * BLOCK, BLOCK), BLOCK)

    def to_sibling(j):
        return remote(pa.at[j, theirs_at, :], sib.at[j], sib_send, sib_recv.at[j], sibling)

    def to_owner(j):
        device = {"feat": lax.rem(x + ahead(j), NX) * NC + c}
        return remote(xs.at[j], xr.at[j], x_send, x_recv, device)

    wait_all(proj_v, in_sem.at[0])

    def step(j, carry):
        wait_all(tokens_v.at[j], chunk_sem.at[j])
        pa[j, :, 0:K] = dot(tokens_v[j, 0], proj_v[0])
        pa[j, :, K:2 * K] = dot(tokens_v[j, 1], proj_v[1])

        @pl.when(j == 0)
        def _():
            pl.semaphore_wait(barrier, NF + NY + NZ - 3)
            for k in Y_FAR:
                pl.semaphore_signal(plane, inc=1, device_id=rows_peer(z, y_at(k)))

        to_sibling(j).start()

        @pl.when(j > 0)
        def _():
            to_sibling(j - 1).wait_recv()
            xs[j - 1] = (pa[j - 1, mine_at, :] + sib[j - 1]).astype(X_DT)
            to_owner(j - 1).start()

        return carry

    lax.fori_loop(0, NX, step, 0)
    for copy in small + late:
        copy.start()
    sent += [(sib, sib_send), (xs.at[0:NX - 1], x_send)]
    to_sibling(NX - 1).wait_recv()

    for copy in small:
        copy.wait()
    doc, lane = iota((K, K), 0), iota((K, K), 1)
    count_row = jnp.broadcast_to(counts_v[...].astype(F32), (K, K))
    start = jnp.sum(jnp.where(lane < doc, count_row, 0.0), axis=1, keepdims=True)
    count = jnp.sum(jnp.where(lane == doc, count_row, 0.0), axis=1, keepdims=True)
    q = iota((DOCS, NF * NR), 1)
    block = (((q & 31) << 3) | (q >> 5)).astype(F32)
    member[...] = jnp.where((start <= block) & (block < start + count), 1.0, 0.0).astype(BF)
    mine = (r * NF + f).astype(F32)
    owner = jnp.sum(jnp.where(start <= mine, 1.0, 0.0), axis=0, keepdims=True) - 1.0
    same = jnp.where(ids_v[pl.ds(f, 1), :].astype(F32) == owner, 1.0, 0.0)
    keep = jnp.sum(jnp.where(lane == doc, jnp.broadcast_to(same, (K, K)), 0.0), axis=1, keepdims=True)
    columns[0] = jnp.broadcast_to(keep, (K, K))
    columns[1] = jnp.broadcast_to(count, (K, K))
    perms[0] = one_hot_rows(lambda q: (q & 31) * 4 + (q >> 5))

    total = pa[NX - 1, mine_at, :] + sib[NX - 1]
    wait_all(xr.at[0:NX - 1], x_recv)
    for j in range(NX - 1):
        total = total + xr[j].astype(F32)

    gmask = jnp.where(columns[0] > 0.5, total[:, K:2 * K], 0.0)
    blocksum = jnp.dot(
        gmask.T, total[:, 0:K], precision=lax.Precision.HIGHEST, preferred_element_type=F32
    )
    s1[...] = blocksum.astype(B_DT).reshape(NR, 4, K)
    got = {}
    pl.semaphore_wait(plane, NY - 1)
    for dz, dy in R_FAR:
        there = z_at(dz) * NY + y_at(dy)
        send(s1.at[there], r1.at[r], b1_send, b1_recv, {"rows": there})
    sent.append((s1.at[0:NR - 1], b1_send))
    r1[r] = s1[r]
    wait_all(r1.at[0:NR - 1], b1_recv)

    turned = dot(perms[0], r1[...].reshape(K, K).astype(BF)).astype(BF)
    ag_at = pl.ds(pl.multiple_of(f * NR, NR), NR)
    for k in range(4):
        ag[k, ag_at, :] = turned[NR * k:NR * k + NR]

    def share(at, k, device):
        return send(ag.at[:, at, :], ag.at[:, at, :], ag_send, ag_recv.at[k], device)

    for k in X_FAR:
        got[k] = share(ag_at, k, feat_at(NC * k))
    share(ag_at, 0, sibling)
    for k in X_FAR[::-1]:
        got[k].wait_recv()
        at = pl.ds(pl.multiple_of(lax.rem(f + NF - NC * k, NF) * NR, NR), NR)
        share(at, 0, sibling)
    sent.append((ag.at[:, 0:(NF - 1) * NR, :], ag_send))
    wait_all(inv_v, in_sem.at[4])
    wait_all(train_v, in_sem.at[5])
    wait_all(ag.at[:, 0:NX * NR, :], ag_recv.at[0])

    for k in range(4):
        dg[:, K * k:K * k + K] = (dot(member[...], ag[k]) / columns[1]).astype(BF)

    for k in Y_FAR:
        s3[k] = dot(dg[...], inv_v[k]).astype(BF)
        send(s3.at[k], r3.at[k], c1_send, c1_recv, rows_peer(z, y_at(k)))
    sent.append((s3.at[1:NY], c1_send))
    own[...] = dot(dg[...], inv_v[0])
    for k in range(4):
        at = slice(K * k, K * k + K)
        own[:, at] += jnp.where(z == f, dg[:, at].astype(F32) * diag_v[k:k + 1, :], 0.0)
    wait_all(r3.at[1:NY], c1_recv)
    own[...] = own[...] + r3[1].astype(F32) + r3[3].astype(F32) + r3[2].astype(F32)
    s4[...] = own[...].astype(BF)
    for k in Z_FAR:
        at = pl.ds(pl.multiple_of(z_at(k) * 16, 16), 16)
        send(s4.at[at, :], r4.at[k], c2_send, c2_recv, rows_peer(z_at(k), y))
    sent.append((s4.at[0:16 * (NZ - 1), :], c2_send))
    here = pl.ds(pl.multiple_of(z * 16, 16), 16)
    piece = own[here, :]
    wait_all(r4.at[1:NZ], c2_recv)
    for k in Z_NEAR:
        piece = piece + r4[k].astype(F32)
    pc[0, here, :] = piece.astype(BF)

    gather = {}

    def forward(at):
        for k in Y_FAR:
            send(pc.at[0, at, :], pc.at[k, at, :], p2_send, p2_recv.at[k], rows_peer(z, y_at(k)))

    for k in Z_FAR:
        gather[k] = send(
            pc.at[0, here, :], pc.at[0, here, :], p1_send, p1_recv.at[k], rows_peer(z_at(k), y)
        )
    forward(here)
    for k in Z_NEAR:
        gather[k].wait_recv()
        forward(pl.ds(pl.multiple_of(z_at(NZ - k) * 16, 16), 16))
    sent += [(pc.at[0, 0:16 * (NZ - 1), :], p1_send), (pc.at[0:NY - 1], p2_send)]
    acc[...] = dot_nt(pc[0], train_v[0])
    for k in Y_NEAR:
        wait_all(pc.at[k], p2_recv.at[k])
        acc[...] += dot_nt(pc[k], train_v[k])

    for k in range(NF):
        s5[k] = acc[16 * k:16 * k + 16, :].astype(D_DT)
    for k in F_FAR:
        send(s5.at[lax.rem(f + k, NF)], r5.at[k], d_send, d_recv, feat_at(k))
    sent.append((s5.at[1:NF], d_send))
    scores = acc[pl.ds(pl.multiple_of(f * 16, 16), 16), :]
    wait_all(r5.at[1:NF], d_recv)
    for k in F_FAR[::-1]:
        scores = scores + r5[k].astype(F32)
    out[...] = scores
    finish()


def per_device(acts, grads_out, proj_in, proj_out, doc_ids, block_counts, inverse_dense, inverse_diag, train_grads):
    def vmem(*shape, dtype=BF):
        return pltpu.VMEM(shape, dtype)

    dma = pltpu.SemaphoreType.DMA
    scratch = [
        vmem(4, 2, 256, 2048), vmem(2, 2048, K),
        vmem(8, 128, dtype=I32), vmem(1, 128, dtype=I32),
        vmem(4, 512, 512), vmem(4, 128, dtype=F32), vmem(4, 512, 512),
        vmem(DOCS, 256), vmem(1, K, K), vmem(2, K, K, dtype=F32),
        vmem(4, 256, 256, dtype=F32), vmem(4, 128, 256, dtype=F32),
        vmem(4, 128, 256, dtype=X_DT), vmem(4, 128, 256, dtype=X_DT),
        vmem(NR, 4, K, dtype=B_DT), vmem(NR, 4, K, dtype=B_DT),
        vmem(4, 256, K), vmem(128, 512),
        vmem(4, 128, 512), vmem(4, 128, 512), vmem(128, 512, dtype=F32),
        vmem(128, 512), vmem(8, 16, 512), vmem(4, 128, 512), vmem(128, 512, dtype=F32),
        vmem(8, 16, 512, dtype=D_DT), vmem(8, 16, 512, dtype=D_DT),
        dma((6,)), dma((NX,)), pltpu.SemaphoreType.REGULAR,
        dma(()), dma((NX,)), dma(()), dma(()), dma(()), dma(()), dma(()), dma((NX,)),
        dma(()), dma(()), dma(()), dma(()), dma(()), dma((NZ,)), dma(()), dma((NY,)),
        dma(()), dma(()),
    ]
    hbm = pl.BlockSpec(memory_space=pl.ANY)
    return pl.pallas_call(
        kernel,
        out_shape=jax.ShapeDtypeStruct((16, 512), F32),
        in_specs=[hbm] * 9,
        out_specs=pl.BlockSpec(memory_space=pltpu.VMEM),
        scratch_shapes=scratch,
        compiler_params=pltpu.CompilerParams(
            collective_id=0, has_side_effects=True, vmem_limit_bytes=60 * 1024 * 1024
        ),
        name="influence",
    )(
        acts, grads_out, proj_in, proj_out,
        doc_ids.reshape(8, 128), block_counts.reshape(1, 128),
        inverse_dense, inverse_diag.reshape(4, 128), train_grads,
    )


def solution(mesh):
    in_specs = (
        P("rows", "feat"),
        P("rows", "feat"),
        P("feat", None),
        P("feat", None),
        P("rows"),
        P(),
        P("rows", "feat"),
        P("rows"),
        P("rows", "feat"),
    )
    return jax.shard_map(
        per_device, mesh=mesh, in_specs=in_specs, out_specs=P("feat", "rows"), check_vma=False
    )
```

```python
import jax
import jax.numpy as jnp
from jax import lax
from jax.experimental import pallas as pl
from jax.experimental.pallas import tpu as pltpu
from jax.sharding import PartitionSpec as P

BF = jnp.bfloat16
F32 = jnp.float32
I32 = jnp.int32

NX, NC, NY, NZ = 4, 2, 4, 8
NF = NX * NC
NR = NZ * NY
BLOCK = 128
K = 128
DOCS = 128
Y_FAR = (2, 1, 3)
Y_NEAR = (1, 3, 2)
Z_FAR = (4, 3, 5, 2, 6, 1, 7)
Z_NEAR = (1, 7, 2, 6, 3, 5, 4)
F_FAR = (4, 5, 3, 2, 6, 7, 1)
X_FAR = (2, 1, 3)
R_FAR = sorted(
    ((dz, dy) for dz in range(NZ) for dy in range(NY) if dz or dy),
    key=lambda d: -min(d[0], NZ - d[0]) - min(d[1], NY - d[1]),
)
X_DT = BF
B_DT = BF
D_DT = BF


def iota(shape, dim):
    return lax.broadcasted_iota(I32, shape, dim)


def one_hot_rows(source_of):
    q = iota((K, K), 0)
    return (iota((K, K), 1) == source_of(q)).astype(F32).astype(BF)


def dot(a, b):
    return jnp.dot(a, b, preferred_element_type=F32)


def dot_nt(a, b):
    return lax.dot_general(a, b, (((1,), (1,)), ((), ())), preferred_element_type=F32)


def kernel(
    acts, grads, pin, pout, ids, counts, inv, diag, train,
    out,
    tokens_v, proj_v, ids_v, counts_v, inv_v, diag_v, train_v,
    member, perms, columns,
    pa, sib, xs, xr, s1, r1, ag, dg, s3, r3, own, s4, r4, pc, acc, s5, r5,
    in_sem, chunk_sem, plane,
    sib_send, sib_recv, x_send, x_recv, b1_send, b1_recv,
    ag_send, ag_recv, c1_send, c1_recv, c2_send, c2_recv, p1_send, p1_recv,
    p2_send, p2_recv, d_send, d_recv,
):
    f = lax.axis_index("feat")
    r = lax.axis_index("rows")
    x, c = f // NC, f % NC
    z, y = r // NY, r % NY

    def feat_at(k):
        return {"feat": lax.rem(f + k, NF)}

    def y_at(k):
        return lax.rem(y + k, NY)

    def z_at(k):
        return lax.rem(z + k, NZ)

    def rows_peer(zp, yp):
        return {"rows": zp * NY + yp}

    sibling = {"feat": x * NC + (1 - c)}

    projections = [
        pltpu.make_async_copy(pin, proj_v.at[0], in_sem.at[0]),
        pltpu.make_async_copy(pout, proj_v.at[1], in_sem.at[0]),
    ]
    for copy in projections:
        copy.start()

    def ahead(j):
        return jnp.where(j == 0, 2, jnp.where(j == 1, 1, jnp.where(j == 2, 3, 0)))

    def chunk(j):
        at = pl.ds(pl.multiple_of(lax.rem(x + ahead(j), NX) * 256, 256), 256)
        return (
            pltpu.make_async_copy(acts.at[at, :], tokens_v.at[j, 0], chunk_sem.at[j]),
            pltpu.make_async_copy(grads.at[at, :], tokens_v.at[j, 1], chunk_sem.at[j]),
        )

    for j in range(NX):
        for copy in chunk(j):
            copy.start()
    small = [
        pltpu.make_async_copy(counts, counts_v, in_sem.at[1]),
        pltpu.make_async_copy(ids, ids_v, in_sem.at[2]),
        pltpu.make_async_copy(diag, diag_v, in_sem.at[3]),
    ]
    late = []
    for k in range(NY):
        at = pl.ds(pl.multiple_of(y_at(k) * 512, 512), 512)
        late.append(pltpu.make_async_copy(inv.at[:, at], inv_v.at[k], in_sem.at[4]))
    for k in range(NY):
        at = pl.ds(pl.multiple_of(y_at(NY - k) * 512, 512), 512)
        late.append(pltpu.make_async_copy(train.at[:, at], train_v.at[k], in_sem.at[5]))

    barrier = pltpu.get_barrier_semaphore()
    for k in range(1, NF):
        pl.semaphore_signal(barrier, inc=1, device_id=feat_at(k))
    for k in Z_FAR:
        pl.semaphore_signal(barrier, inc=1, device_id=rows_peer(z_at(k), y))
    for k in Y_FAR:
        pl.semaphore_signal(barrier, inc=1, device_id=rows_peer(z, y_at(k)))

    sent = []

    def remote(src, dst, ssem, rsem, device):
        return pltpu.make_async_remote_copy(
            src_ref=src, dst_ref=dst, send_sem=ssem, recv_sem=rsem,
            device_id=device, device_id_type=pl.DeviceIdType.MESH,
        )

    def send(*args):
        copy = remote(*args)
        copy.start()
        return copy

    def wait_all(ref, sem):
        pltpu.make_async_copy(ref, ref, sem).wait()

    def finish():
        for ref, sem in sent:
            wait_all(ref, sem)

    mine_at = pl.ds(pl.multiple_of(c * BLOCK, BLOCK), BLOCK)
    theirs_at = pl.ds(pl.multiple_of((1 - c) * BLOCK, BLOCK), BLOCK)

    def to_sibling(j):
        return remote(pa.at[j, theirs_at, :], sib.at[j], sib_send, sib_recv.at[j], sibling)

    def to_owner(j):
        device = {"feat": lax.rem(x + ahead(j), NX) * NC + c}
        return remote(xs.at[j], xr.at[j], x_send, x_recv, device)

    wait_all(proj_v, in_sem.at[0])

    def step(j, carry):
        wait_all(tokens_v.at[j], chunk_sem.at[j])
        pa[j, :, 0:K] = dot(tokens_v[j, 0], proj_v[0])
        pa[j, :, K:2 * K] = dot(tokens_v[j, 1], proj_v[1])

        @pl.when(j == 0)
        def _():
            pl.semaphore_wait(barrier, NF + NY + NZ - 3)
            for k in Y_FAR:
                pl.semaphore_signal(plane, inc=1, device_id=rows_peer(z, y_at(k)))

        to_sibling(j).start()

        @pl.when(j > 0)
        def _():
            to_sibling(j - 1).wait_recv()
            xs[j - 1] = (pa[j - 1, mine_at, :] + sib[j - 1]).astype(X_DT)
            to_owner(j - 1).start()

        return carry

    lax.fori_loop(0, NX, step, 0)
    for copy in small + late:
        copy.start()
    sent += [(sib, sib_send), (xs.at[0:NX - 1], x_send)]
    to_sibling(NX - 1).wait_recv()

    for copy in small:
        copy.wait()
    doc, lane = iota((K, K), 0), iota((K, K), 1)
    count_row = jnp.broadcast_to(counts_v[...].astype(F32), (K, K))
    start = jnp.sum(jnp.where(lane < doc, count_row, 0.0), axis=1, keepdims=True)
    count = jnp.sum(jnp.where(lane == doc, count_row, 0.0), axis=1, keepdims=True)
    q = iota((DOCS, NF * NR), 1)
    block = (((q & 31) << 3) | (q >> 5)).astype(F32)
    member[...] = jnp.where((start <= block) & (block < start + count), 1.0, 0.0).astype(BF)
    mine = (r * NF + f).astype(F32)
    owner = jnp.sum(jnp.where(start <= mine, 1.0, 0.0), axis=0, keepdims=True) - 1.0
    same = jnp.where(ids_v[pl.ds(f, 1), :].astype(F32) == owner, 1.0, 0.0)
    keep = jnp.sum(jnp.where(lane == doc, jnp.broadcast_to(same, (K, K)), 0.0), axis=1, keepdims=True)
    columns[0] = jnp.broadcast_to(keep, (K, K))
    columns[1] = jnp.broadcast_to(count, (K, K))
    perms[0] = one_hot_rows(lambda q: (q & 31) * 4 + (q >> 5))

    total = pa[NX - 1, mine_at, :] + sib[NX - 1]
    wait_all(xr.at[0:NX - 1], x_recv)
    for j in range(NX - 1):
        total = total + xr[j].astype(F32)

    gmask = jnp.where(columns[0] > 0.5, total[:, K:2 * K], 0.0)
    blocksum = jnp.dot(
        gmask.T, total[:, 0:K], precision=lax.Precision.HIGHEST, preferred_element_type=F32
    )
    s1[...] = blocksum.astype(B_DT).reshape(NR, 4, K)
    got = {}
    pl.semaphore_wait(plane, NY - 1)
    for dz, dy in R_FAR:
        there = z_at(dz) * NY + y_at(dy)
        send(s1.at[there], r1.at[r], b1_send, b1_recv, {"rows": there})
    sent.append((s1.at[0:NR - 1], b1_send))
    r1[r] = s1[r]
    wait_all(r1.at[0:NR - 1], b1_recv)

    turned = dot(perms[0], r1[...].reshape(K, K).astype(BF)).astype(BF)
    ag_at = pl.ds(pl.multiple_of(f * NR, NR), NR)
    for k in range(4):
        ag[k, ag_at, :] = turned[NR * k:NR * k + NR]

    def share(at, k, device):
        return send(ag.at[:, at, :], ag.at[:, at, :], ag_send, ag_recv.at[k], device)

    for k in F_FAR:
        share(ag_at, 0, feat_at(k))
    sent.append((ag.at[:, 0:(NF - 1) * NR, :], ag_send))
    wait_all(inv_v, in_sem.at[4])
    wait_all(train_v, in_sem.at[5])
    wait_all(ag.at[:, 0:(NF - 1) * NR, :], ag_recv.at[0])

    for k in range(4):
        dg[:, K * k:K * k + K] = (dot(member[...], ag[k]) / columns[1]).astype(BF)

    for k in Y_FAR:
        s3[k] = dot(dg[...], inv_v[k]).astype(BF)
        send(s3.at[k], r3.at[k], c1_send, c1_recv, rows_peer(z, y_at(k)))
    sent.append((s3.at[1:NY], c1_send))
    own[...] = dot(dg[...], inv_v[0])
    for k in range(4):
        at = slice(K * k, K * k + K)
        own[:, at] += jnp.where(z == f, dg[:, at].astype(F32) * diag_v[k:k + 1, :], 0.0)
    wait_all(r3.at[1:NY], c1_recv)
    own[...] = own[...] + r3[1].astype(F32) + r3[3].astype(F32) + r3[2].astype(F32)
    s4[...] = own[...].astype(BF)
    for k in Z_FAR:
        at = pl.ds(pl.multiple_of(z_at(k) * 16, 16), 16)
        send(s4.at[at, :], r4.at[k], c2_send, c2_recv, rows_peer(z_at(k), y))
    sent.append((s4.at[0:16 * (NZ - 1), :], c2_send))
    here = pl.ds(pl.multiple_of(z * 16, 16), 16)
    piece = own[here, :]
    wait_all(r4.at[1:NZ], c2_recv)
    for k in Z_NEAR:
        piece = piece + r4[k].astype(F32)
    pc[0, here, :] = piece.astype(BF)

    gather = {}

    def forward(at):
        for k in Y_FAR:
            send(pc.at[0, at, :], pc.at[k, at, :], p2_send, p2_recv.at[k], rows_peer(z, y_at(k)))

    for k in Z_NEAR:
        gather[k] = send(
            pc.at[0, here, :], pc.at[0, here, :], p1_send, p1_recv.at[k], rows_peer(z_at(k), y)
        )
    forward(here)
    for k in Z_NEAR:
        gather[k].wait_recv()
        forward(pl.ds(pl.multiple_of(z_at(NZ - k) * 16, 16), 16))
    sent += [(pc.at[0, 0:16 * (NZ - 1), :], p1_send), (pc.at[0:NY - 1], p2_send)]
    acc[...] = dot_nt(pc[0], train_v[0])
    for k in Y_NEAR:
        wait_all(pc.at[k], p2_recv.at[k])
        acc[...] += dot_nt(pc[k], train_v[k])

    for k in range(NF):
        s5[k] = acc[16 * k:16 * k + 16, :].astype(D_DT)
    for k in F_FAR:
        send(s5.at[lax.rem(f + k, NF)], r5.at[k], d_send, d_recv, feat_at(k))
    sent.append((s5.at[1:NF], d_send))
    scores = acc[pl.ds(pl.multiple_of(f * 16, 16), 16), :]
    wait_all(r5.at[1:NF], d_recv)
    for k in F_FAR[::-1]:
        scores = scores + r5[k].astype(F32)
    out[...] = scores
    finish()


def per_device(acts, grads_out, proj_in, proj_out, doc_ids, block_counts, inverse_dense, inverse_diag, train_grads):
    def vmem(*shape, dtype=BF):
        return pltpu.VMEM(shape, dtype)

    dma = pltpu.SemaphoreType.DMA
    scratch = [
        vmem(4, 2, 256, 2048), vmem(2, 2048, K),
        vmem(8, 128, dtype=I32), vmem(1, 128, dtype=I32),
        vmem(4, 512, 512), vmem(4, 128, dtype=F32), vmem(4, 512, 512),
        vmem(DOCS, 256), vmem(1, K, K), vmem(2, K, K, dtype=F32),
        vmem(4, 256, 256, dtype=F32), vmem(4, 128, 256, dtype=F32),
        vmem(4, 128, 256, dtype=X_DT), vmem(4, 128, 256, dtype=X_DT),
        vmem(NR, 4, K, dtype=B_DT), vmem(NR, 4, K, dtype=B_DT),
        vmem(4, 256, K), vmem(128, 512),
        vmem(4, 128, 512), vmem(4, 128, 512), vmem(128, 512, dtype=F32),
        vmem(128, 512), vmem(8, 16, 512), vmem(4, 128, 512), vmem(128, 512, dtype=F32),
        vmem(8, 16, 512, dtype=D_DT), vmem(8, 16, 512, dtype=D_DT),
        dma((6,)), dma((NX,)), pltpu.SemaphoreType.REGULAR,
        dma(()), dma((NX,)), dma(()), dma(()), dma(()), dma(()), dma(()), dma((NX,)),
        dma(()), dma(()), dma(()), dma(()), dma(()), dma((NZ,)), dma(()), dma((NY,)),
        dma(()), dma(()),
    ]
    hbm = pl.BlockSpec(memory_space=pl.ANY)
    return pl.pallas_call(
        kernel,
        out_shape=jax.ShapeDtypeStruct((16, 512), F32),
        in_specs=[hbm] * 9,
        out_specs=pl.BlockSpec(memory_space=pltpu.VMEM),
        scratch_shapes=scratch,
        compiler_params=pltpu.CompilerParams(
            collective_id=0, has_side_effects=True, vmem_limit_bytes=60 * 1024 * 1024
        ),
        name="influence",
    )(
        acts, grads_out, proj_in, proj_out,
        doc_ids.reshape(8, 128), block_counts.reshape(1, 128),
        inverse_dense, inverse_diag.reshape(4, 128), train_grads,
    )


def solution(mesh):
    in_specs = (
        P("rows", "feat"),
        P("rows", "feat"),
        P("feat", None),
        P("feat", None),
        P("rows"),
        P(),
        P("rows", "feat"),
        P("rows"),
        P("rows", "feat"),
    )
    return jax.shard_map(
        per_device, mesh=mesh, in_specs=in_specs, out_specs=P("feat", "rows"), check_vma=False
    )
```

```python
import jax
import jax.numpy as jnp
from jax import lax
from jax.experimental import pallas as pl
from jax.experimental.pallas import tpu as pltpu
from jax.sharding import PartitionSpec as P

BF = jnp.bfloat16
F32 = jnp.float32
I32 = jnp.int32

NX, NC, NY, NZ = 4, 2, 4, 8
NF = NX * NC
NR = NZ * NY
BLOCK = 128
K = 128
DOCS = 128
Y_FAR = (2, 1, 3)
Y_NEAR = (1, 3, 2)
Z_FAR = (4, 3, 5, 2, 6, 1, 7)
Z_NEAR = (1, 7, 2, 6, 3, 5, 4)
F_FAR = (4, 5, 3, 2, 6, 7, 1)
X_FAR = (2, 1, 3)
R_FAR = sorted(
    ((dz, dy) for dz in range(NZ) for dy in range(NY) if dz or dy),
    key=lambda d: -min(d[0], NZ - d[0]) - min(d[1], NY - d[1]),
)
X_DT = BF
B_DT = BF
D_DT = BF


def iota(shape, dim):
    return lax.broadcasted_iota(I32, shape, dim)


def one_hot_rows(source_of):
    q = iota((K, K), 0)
    return (iota((K, K), 1) == source_of(q)).astype(F32).astype(BF)


def dot(a, b):
    return jnp.dot(a, b, preferred_element_type=F32)


def dot_nt(a, b):
    return lax.dot_general(a, b, (((1,), (1,)), ((), ())), preferred_element_type=F32)


def kernel(
    acts, grads, pin, pout, ids, counts, inv, diag, train,
    out,
    tokens_v, proj_v, ids_v, counts_v, inv_v, diag_v, train_v,
    member, perms, columns,
    pa, sib, xs, xr, s1, r1, ag, dg, s3, r3, own, s4, r4, pc, acc, s5, r5,
    in_sem, chunk_sem, plane,
    sib_send, sib_recv, x_send, x_recv, b1_send, b1_recv,
    ag_send, ag_recv, c1_send, c1_recv, c2_send, c2_recv, p1_send, p1_recv,
    p2_send, p2_recv, d_send, d_recv,
):
    f = lax.axis_index("feat")
    r = lax.axis_index("rows")
    x, c = f // NC, f % NC
    z, y = r // NY, r % NY

    def feat_at(k):
        return {"feat": lax.rem(f + k, NF)}

    def y_at(k):
        return lax.rem(y + k, NY)

    def z_at(k):
        return lax.rem(z + k, NZ)

    def rows_peer(zp, yp):
        return {"rows": zp * NY + yp}

    sibling = {"feat": x * NC + (1 - c)}

    projections = [
        pltpu.make_async_copy(pin, proj_v.at[0], in_sem.at[0]),
        pltpu.make_async_copy(pout, proj_v.at[1], in_sem.at[0]),
    ]
    for copy in projections:
        copy.start()

    def ahead(j):
        return jnp.where(j == 0, 2, jnp.where(j == 1, 1, jnp.where(j == 2, 3, 0)))

    def chunk(j):
        at = pl.ds(pl.multiple_of(lax.rem(x + ahead(j), NX) * 256, 256), 256)
        return (
            pltpu.make_async_copy(acts.at[at, :], tokens_v.at[j, 0], chunk_sem.at[j]),
            pltpu.make_async_copy(grads.at[at, :], tokens_v.at[j, 1], chunk_sem.at[j]),
        )

    for j in range(NX):
        for copy in chunk(j):
            copy.start()
    small = [
        pltpu.make_async_copy(counts, counts_v, in_sem.at[1]),
        pltpu.make_async_copy(ids, ids_v, in_sem.at[2]),
        pltpu.make_async_copy(diag, diag_v, in_sem.at[3]),
    ]
    for copy in small:
        copy.start()
    late = []
    for k in range(NY):
        at = pl.ds(pl.multiple_of(y_at(k) * 512, 512), 512)
        late.append(pltpu.make_async_copy(inv.at[:, at], inv_v.at[k], in_sem.at[4]))
    for k in range(NY):
        at = pl.ds(pl.multiple_of(y_at(NY - k) * 512, 512), 512)
        late.append(pltpu.make_async_copy(train.at[:, at], train_v.at[k], in_sem.at[5]))

    barrier = pltpu.get_barrier_semaphore()
    for k in range(1, NF):
        pl.semaphore_signal(barrier, inc=1, device_id=feat_at(k))
    for k in Z_FAR:
        pl.semaphore_signal(barrier, inc=1, device_id=rows_peer(z_at(k), y))
    for k in Y_FAR:
        pl.semaphore_signal(barrier, inc=1, device_id=rows_peer(z, y_at(k)))

    sent = []

    def remote(src, dst, ssem, rsem, device):
        return pltpu.make_async_remote_copy(
            src_ref=src, dst_ref=dst, send_sem=ssem, recv_sem=rsem,
            device_id=device, device_id_type=pl.DeviceIdType.MESH,
        )

    def send(*args):
        copy = remote(*args)
        copy.start()
        return copy

    def wait_all(ref, sem):
        pltpu.make_async_copy(ref, ref, sem).wait()

    def finish():
        for ref, sem in sent:
            wait_all(ref, sem)

    mine_at = pl.ds(pl.multiple_of(c * BLOCK, BLOCK), BLOCK)
    theirs_at = pl.ds(pl.multiple_of((1 - c) * BLOCK, BLOCK), BLOCK)

    def to_sibling(j):
        return remote(pa.at[j, theirs_at, :], sib.at[j], sib_send, sib_recv.at[j], sibling)

    def to_owner(j):
        device = {"feat": lax.rem(x + ahead(j), NX) * NC + c}
        return remote(xs.at[j], xr.at[j], x_send, x_recv, device)

    wait_all(proj_v, in_sem.at[0])

    def step(j, carry):
        wait_all(tokens_v.at[j], chunk_sem.at[j])
        pa[j, :, 0:K] = dot(tokens_v[j, 0], proj_v[0])
        pa[j, :, K:2 * K] = dot(tokens_v[j, 1], proj_v[1])

        @pl.when(j == 0)
        def _():
            pl.semaphore_wait(barrier, NF + NY + NZ - 3)
            for k in Y_FAR:
                pl.semaphore_signal(plane, inc=1, device_id=rows_peer(z, y_at(k)))

        to_sibling(j).start()

        @pl.when(j > 0)
        def _():
            to_sibling(j - 1).wait_recv()
            xs[j - 1] = (pa[j - 1, mine_at, :] + sib[j - 1]).astype(X_DT)
            to_owner(j - 1).start()

        return carry

    lax.fori_loop(0, NX, step, 0)
    for copy in late:
        copy.start()
    sent += [(sib, sib_send), (xs.at[0:NX - 1], x_send)]
    to_sibling(NX - 1).wait_recv()

    for copy in small:
        copy.wait()
    doc, lane = iota((K, K), 0), iota((K, K), 1)
    count_row = jnp.broadcast_to(counts_v[...].astype(F32), (K, K))
    start = jnp.sum(jnp.where(lane < doc, count_row, 0.0), axis=1, keepdims=True)
    count = jnp.sum(jnp.where(lane == doc, count_row, 0.0), axis=1, keepdims=True)
    q = iota((DOCS, NF * NR), 1)
    block = (((q & 31) << 3) | (q >> 5)).astype(F32)
    member[...] = jnp.where((start <= block) & (block < start + count), 1.0, 0.0).astype(BF)
    mine = (r * NF + f).astype(F32)
    owner = jnp.sum(jnp.where(start <= mine, 1.0, 0.0), axis=0, keepdims=True) - 1.0
    same = jnp.where(ids_v[pl.ds(f, 1), :].astype(F32) == owner, 1.0, 0.0)
    keep = jnp.sum(jnp.where(lane == doc, jnp.broadcast_to(same, (K, K)), 0.0), axis=1, keepdims=True)
    columns[0] = jnp.broadcast_to(keep, (K, K))
    columns[1] = jnp.broadcast_to(count, (K, K))
    perms[0] = one_hot_rows(lambda q: (q & 31) * 4 + (q >> 5))

    total = pa[NX - 1, mine_at, :] + sib[NX - 1]
    wait_all(xr.at[0:NX - 1], x_recv)
    for j in range(NX - 1):
        total = total + xr[j].astype(F32)

    gmask = jnp.where(columns[0] > 0.5, total[:, K:2 * K], 0.0)
    blocksum = jnp.dot(
        gmask.T, total[:, 0:K], precision=lax.Precision.HIGHEST, preferred_element_type=F32
    )
    s1[...] = blocksum.astype(B_DT).reshape(NR, 4, K)
    got = {}
    pl.semaphore_wait(plane, NY - 1)
    for dz, dy in R_FAR:
        there = z_at(dz) * NY + y_at(dy)
        send(s1.at[there], r1.at[r], b1_send, b1_recv, {"rows": there})
    sent.append((s1.at[0:NR - 1], b1_send))
    r1[r] = s1[r]
    wait_all(r1.at[0:NR - 1], b1_recv)

    turned = dot(perms[0], r1[...].reshape(K, K).astype(BF)).astype(BF)
    ag_at = pl.ds(pl.multiple_of(f * NR, NR), NR)
    for k in range(4):
        ag[k, ag_at, :] = turned[NR * k:NR * k + NR]

    def share(at, k, device):
        return send(ag.at[:, at, :], ag.at[:, at, :], ag_send, ag_recv.at[k], device)

    for k in F_FAR:
        share(ag_at, 0, feat_at(k))
    sent.append((ag.at[:, 0:(NF - 1) * NR, :], ag_send))
    wait_all(inv_v, in_sem.at[4])
    wait_all(train_v, in_sem.at[5])
    wait_all(ag.at[:, 0:(NF - 1) * NR, :], ag_recv.at[0])

    for k in range(4):
        dg[:, K * k:K * k + K] = (dot(member[...], ag[k]) / columns[1]).astype(BF)

    for k in Y_FAR:
        s3[k] = dot(dg[...], inv_v[k]).astype(BF)
        send(s3.at[k], r3.at[k], c1_send, c1_recv, rows_peer(z, y_at(k)))
    sent.append((s3.at[1:NY], c1_send))
    own[...] = dot(dg[...], inv_v[0])
    for k in range(4):
        at = slice(K * k, K * k + K)
        own[:, at] += jnp.where(z == f, dg[:, at].astype(F32) * diag_v[k:k + 1, :], 0.0)
    wait_all(r3.at[1:NY], c1_recv)
    own[...] = own[...] + r3[1].astype(F32) + r3[3].astype(F32) + r3[2].astype(F32)
    s4[...] = own[...].astype(BF)
    for k in Z_FAR:
        at = pl.ds(pl.multiple_of(z_at(k) * 16, 16), 16)
        send(s4.at[at, :], r4.at[k], c2_send, c2_recv, rows_peer(z_at(k), y))
    sent.append((s4.at[0:16 * (NZ - 1), :], c2_send))
    here = pl.ds(pl.multiple_of(z * 16, 16), 16)
    piece = own[here, :]
    wait_all(r4.at[1:NZ], c2_recv)
    for k in Z_NEAR:
        piece = piece + r4[k].astype(F32)
    pc[0, here, :] = piece.astype(BF)

    gather = {}

    def forward(at):
        for k in Y_FAR:
            send(pc.at[0, at, :], pc.at[k, at, :], p2_send, p2_recv.at[k], rows_peer(z, y_at(k)))

    for k in Z_NEAR:
        gather[k] = send(
            pc.at[0, here, :], pc.at[0, here, :], p1_send, p1_recv.at[k], rows_peer(z_at(k), y)
        )
    forward(here)
    for k in Z_NEAR:
        gather[k].wait_recv()
        forward(pl.ds(pl.multiple_of(z_at(NZ - k) * 16, 16), 16))
    sent += [(pc.at[0, 0:16 * (NZ - 1), :], p1_send), (pc.at[0:NY - 1], p2_send)]
    acc[...] = dot_nt(pc[0], train_v[0])
    for k in Y_NEAR:
        wait_all(pc.at[k], p2_recv.at[k])
        acc[...] += dot_nt(pc[k], train_v[k])

    for k in range(NF):
        s5[k] = acc[16 * k:16 * k + 16, :].astype(D_DT)
    for k in F_FAR:
        send(s5.at[lax.rem(f + k, NF)], r5.at[k], d_send, d_recv, feat_at(k))
    sent.append((s5.at[1:NF], d_send))
    scores = acc[pl.ds(pl.multiple_of(f * 16, 16), 16), :]
    wait_all(r5.at[1:NF], d_recv)
    for k in F_FAR[::-1]:
        scores = scores + r5[k].astype(F32)
    out[...] = scores
    finish()


def per_device(acts, grads_out, proj_in, proj_out, doc_ids, block_counts, inverse_dense, inverse_diag, train_grads):
    def vmem(*shape, dtype=BF):
        return pltpu.VMEM(shape, dtype)

    dma = pltpu.SemaphoreType.DMA
    scratch = [
        vmem(4, 2, 256, 2048), vmem(2, 2048, K),
        vmem(8, 128, dtype=I32), vmem(1, 128, dtype=I32),
        vmem(4, 512, 512), vmem(4, 128, dtype=F32), vmem(4, 512, 512),
        vmem(DOCS, 256), vmem(1, K, K), vmem(2, K, K, dtype=F32),
        vmem(4, 256, 256, dtype=F32), vmem(4, 128, 256, dtype=F32),
        vmem(4, 128, 256, dtype=X_DT), vmem(4, 128, 256, dtype=X_DT),
        vmem(NR, 4, K, dtype=B_DT), vmem(NR, 4, K, dtype=B_DT),
        vmem(4, 256, K), vmem(128, 512),
        vmem(4, 128, 512), vmem(4, 128, 512), vmem(128, 512, dtype=F32),
        vmem(128, 512), vmem(8, 16, 512), vmem(4, 128, 512), vmem(128, 512, dtype=F32),
        vmem(8, 16, 512, dtype=D_DT), vmem(8, 16, 512, dtype=D_DT),
        dma((6,)), dma((NX,)), pltpu.SemaphoreType.REGULAR,
        dma(()), dma((NX,)), dma(()), dma(()), dma(()), dma(()), dma(()), dma((NX,)),
        dma(()), dma(()), dma(()), dma(()), dma(()), dma((NZ,)), dma(()), dma((NY,)),
        dma(()), dma(()),
    ]
    hbm = pl.BlockSpec(memory_space=pl.ANY)
    return pl.pallas_call(
        kernel,
        out_shape=jax.ShapeDtypeStruct((16, 512), F32),
        in_specs=[hbm] * 9,
        out_specs=pl.BlockSpec(memory_space=pltpu.VMEM),
        scratch_shapes=scratch,
        compiler_params=pltpu.CompilerParams(
            collective_id=0, has_side_effects=True, vmem_limit_bytes=60 * 1024 * 1024
        ),
        name="influence",
    )(
        acts, grads_out, proj_in, proj_out,
        doc_ids.reshape(8, 128), block_counts.reshape(1, 128),
        inverse_dense, inverse_diag.reshape(4, 128), train_grads,
    )


def solution(mesh):
    in_specs = (
        P("rows", "feat"),
        P("rows", "feat"),
        P("feat", None),
        P("feat", None),
        P("rows"),
        P(),
        P("rows", "feat"),
        P("rows"),
        P("rows", "feat"),
    )
    return jax.shard_map(
        per_device, mesh=mesh, in_specs=in_specs, out_specs=P("feat", "rows"), check_vma=False
    )
```
